32 devices in a mesh: face: 4 (over x, core), sub: 8 (over z, y).
Axes of the slice: x: 2, y: 2, z: 4, core: 2. Of those that a mesh axis runs over, the one named last changes fastest.
Arguments:
- grid_latent: bfloat16 [16384, 512], P(('face', 'sub')), may hold values from -6 to 6
- mesh_latent: bfloat16 [4096, 512], P(('face', 'sub')), may hold values from -6 to 6
- edge_latent: bfloat16 [32768, 512], P(('face', 'sub')), may hold values from -6 to 6
- mesh_cotangent: bfloat16 [4096, 512], P(('face', 'sub')), may hold values from -6 to 6
- edge_cotangent: bfloat16 [32768, 512], P(('face', 'sub')), may hold values from -6 to 6
- grid_send: int32 [32, 4, 256], P(('face', 'sub')), may hold values from 0 to 511
- grid_slot: int32 [32768], P(('face', 'sub')), may hold values from 0 to 1535, as said below
- grid_target: int32 [32768], P(('face', 'sub')), may hold values from 0 to 127
- mesh_halo: int32 [32, 4, 64], P(('face', 'sub')), may hold values from 0 to 127
- mesh_send: int32 [32, 32, 4], P(('face', 'sub')), may hold values from 0 to 127
- mesh_slot: int32 [32768], P(('face', 'sub')), may hold values from 0 to 511, as said below
- mesh_target: int32 [32768], P(('face', 'sub')), may hold values from 0 to 127
- weights: bfloat16 [10, 512, 512], replicated, may hold values from -0.25 to 0.25
Outputs:
- mesh_update: bfloat16 [4096, 512], P(('face', 'sub'))
- grid_grad: bfloat16 [16384, 512], P(('face', 'sub'))
- mesh_grad: bfloat16 [4096, 512], P(('face', 'sub'))
- edge_grad: bfloat16 [32768, 512], P(('face', 'sub'))
- weight_grads: bfloat16 [10, 512, 512], replicated
The draws below stay inside these ranges and needn't reach their ends.
Inputs may be any that keep to these rules, and one draw needn't show every extreme that they name: grid_slot[e] names the edge device's own 512 grid rows or, above them, the 256 rows listed by each of its four neighbours in direction order. grid_target[e] is local to the edge's device. grid_send[q, k] lists local rows of device q for the device d with nb(d, k) = q; a row may appear in several slots. mesh_slot[e] names the own 128 mesh rows, then the 64 rows listed by each of the four neighbours, then 4 far rows from each device, source major. mesh_target[e] is local to the edge's device. mesh_halo[q, k] lists local rows of device q for its neighbour in direction k. mesh_send[q, d] lists local rows of device q for far edges of device d.
All inputs are finite; a program needn't handle non-finite values.
Results may differ from the reference program's by a relative error of at most 0.016.
Values may be sent and summed in bfloat16 or wider, within the bound.
A program may use at most 128 MiB of HBM per device.

```python
import jax
import jax.numpy as jnp
from jax import lax

LATENT = 512
M_DEV = 128
G_DEV = 512
E1_DEV = 1024
E2_DEV = 1024
HALO_G = 256
HALO_M = 64
CAP_M = 4
PEERS = 32
GRID = 16384
MESH = 4096
E1_TOTAL = 32768
E2_TOTAL = 32768
N_FACE = 4
N_SUB = 8


def draw_grid_slot(key, part):
    count = E1_DEV * PEERS
    choose = jax.random.randint(jax.random.fold_in(key, 11), (count,), 0, 10)
    own = jax.random.randint(jax.random.fold_in(key, 12), (count,), 0, G_DEV)
    near = jax.random.randint(jax.random.fold_in(key, 13), (count,), G_DEV, G_DEV + 4 * HALO_G)
    return jnp.where(choose < 6, own, near).astype(jnp.int32)


def draw_mesh_slot(key, part):
    count = E2_DEV * PEERS
    choose = jax.random.randint(jax.random.fold_in(key, 21), (count,), 0, 6)
    own = jax.random.randint(jax.random.fold_in(key, 22), (count,), 0, M_DEV)
    near = jax.random.randint(jax.random.fold_in(key, 23), (count,), M_DEV, M_DEV + 4 * HALO_M)
    distant = jax.random.randint(jax.random.fold_in(key, 24), (count,), M_DEV + 4 * HALO_M, M_DEV + 4 * HALO_M + CAP_M * PEERS)
    return jnp.where(choose < 3, own, jnp.where(choose < 5, near, distant)).astype(jnp.int32)


def with_ends(result, key, low, high):
    place = [jax.random.randint(jax.random.fold_in(key, axis), (), 0, length) for axis, length in enumerate(result.shape)]
    widest = result.shape.index(max(result.shape))
    beside = place[:widest] + [(place[widest] + 1) % result.shape[widest]] + place[widest + 1:]
    return result.at[tuple(place)].set(low).at[tuple(beside)].set(high)


def levels(rng, shape, split, smallest, largest):
    def one(dim, parts):
        heights = jax.random.uniform(jax.random.fold_in(jax.random.fold_in(rng, 6), dim), (parts,), jnp.float32, smallest / len(split), largest / len(split))
        return jnp.repeat(jnp.exp(heights), shape[dim] // parts).reshape((-1,) + (1,) * (len(shape) - dim - 1))

    gain = one(*split[0])
    for cut in split[1:]:
        gain = gain * one(*cut)
    return gain


def centred(stream_key, dims, width, limit, split=(), held_as=jnp.bfloat16):
    factor_of = levels(stream_key, dims, split, -0.22, 0.18) if split else 1.0
    drawn = jax.random.normal(stream_key, dims, jnp.float32) * width * factor_of
    return jnp.minimum(jnp.maximum(drawn, -limit), limit).astype(held_as)


def setup_inputs(seed: int = 0) -> dict:
    splits = jax.random.split(jax.random.key(seed), 14)
    return {
        "grid_latent": centred(splits[0], (GRID, LATENT), 1.0, 6.0, ((0, 32),)),
        "mesh_latent": centred(splits[1], (MESH, LATENT), 1.0, 6.0, ((0, 32),)),
        "edge_latent": centred(splits[2], (E2_TOTAL, LATENT), 1.0, 6.0, ((0, 32),)),
        "mesh_cotangent": centred(splits[3], (MESH, LATENT), 1.0, 6.0, ((0, 32),)),
        "edge_cotangent": centred(splits[4], (E2_TOTAL, LATENT), 1.0, 6.0, ((0, 32),)),
        "grid_send": with_ends(jax.random.randint(splits[5], (PEERS, 4, HALO_G), 0, G_DEV), jax.random.fold_in(splits[5], 1), 0, G_DEV - 1).astype(jnp.int32),
        "grid_slot": draw_grid_slot(jax.random.fold_in(splits[13], 71), 0),
        "grid_target": with_ends(jax.random.randint(splits[7], (E1_TOTAL,), 0, M_DEV), jax.random.fold_in(splits[7], 1), 0, M_DEV - 1).astype(jnp.int32),
        "mesh_halo": with_ends(jax.random.randint(splits[8], (PEERS, 4, HALO_M), 0, M_DEV), jax.random.fold_in(splits[8], 1), 0, M_DEV - 1).astype(jnp.int32),
        "mesh_send": with_ends(jax.random.randint(splits[9], (PEERS, PEERS, CAP_M), 0, M_DEV), jax.random.fold_in(splits[9], 1), 0, M_DEV - 1).astype(jnp.int32),
        "mesh_slot": draw_mesh_slot(jax.random.fold_in(splits[13], 71), 0),
        "mesh_target": with_ends(jax.random.randint(splits[11], (E2_TOTAL,), 0, M_DEV), jax.random.fold_in(splits[11], 1), 0, M_DEV - 1).astype(jnp.int32),
        "weights": centred(splits[12], (10, LATENT, LATENT), LATENT ** -0.5, 0.25),
    }


norm_eps = 1e-05

def layer_norm(values):
    centre = values - lax.optimization_barrier(jnp.mean(values, axis=-1, keepdims=True))
    spread = lax.optimization_barrier(jnp.mean(centre * centre, axis=-1, keepdims=True))
    return centre * lax.rsqrt(spread + norm_eps)

def layer_norm_back(values, upstream):
    centre = values - lax.optimization_barrier(jnp.mean(values, axis=-1, keepdims=True))
    inverse = lax.rsqrt(lax.optimization_barrier(jnp.mean(centre * centre, axis=-1, keepdims=True)) + norm_eps)
    normed = centre * inverse
    return inverse * (upstream - lax.optimization_barrier(jnp.mean(upstream, axis=-1, keepdims=True)) - normed * lax.optimization_barrier(jnp.mean(upstream * normed, axis=-1, keepdims=True)))

def swish_slope(values):
    sigmoid_values = jax.nn.sigmoid(values)
    return sigmoid_values * (1.0 + values * (1.0 - sigmoid_values))

def product(former, latter):
    return jnp.dot(former, latter, preferred_element_type=jnp.float32)

def outer_sum(former, latter):
    return lax.dot_general(former, latter, (((0,), (0,)), ((), ())), preferred_element_type=jnp.float32)

def back_product(former, latter):
    return lax.dot_general(former, latter, (((1,), (1,)), ((), ())), preferred_element_type=jnp.float32)

def neighbour_device(device, block):
    face_index = device // N_SUB
    sub_index = device % N_SUB
    sub_step = jnp.where(block == 0, -1, jnp.where(block == 1, 1, 0))
    face_step = jnp.where(block == 2, -1, jnp.where(block == 3, 1, 0))
    return ((face_index + face_step) % N_FACE * N_SUB + (sub_index + sub_step) % N_SUB).astype(jnp.int32)

def slot_partials(values, slot_ids, slot_count, local_count):
    sums = jax.ops.segment_sum(values, slot_ids, num_segments=slot_count)
    rounded = lax.optimization_barrier(sums.astype(jnp.bfloat16)).astype(jnp.float32)
    keep = (jnp.arange(slot_count, dtype=jnp.int32) < local_count)[:, None]
    return jnp.where(keep, sums, rounded)

def reference(grid_latent, mesh_latent, edge_latent, mesh_cotangent, edge_cotangent, grid_send, grid_slot, grid_target, mesh_halo, mesh_send, mesh_slot, mesh_target, weights):
    peer_count = N_FACE * N_SUB
    grid_slot_count = G_DEV + 4 * HALO_G
    mesh_slot_count = M_DEV + 4 * HALO_M + CAP_M * peer_count
    device_ids = jnp.arange(peer_count, dtype=jnp.int32)
    grid_slots = grid_slot.reshape(peer_count, E1_DEV)
    grid_targets = grid_target.reshape(peer_count, E1_DEV)
    mesh_slots = mesh_slot.reshape(peer_count, E2_DEV)
    mesh_targets = mesh_target.reshape(peer_count, E2_DEV)
    edge_blocks = edge_latent.reshape(peer_count, E2_DEV, LATENT)
    edge_cots = edge_cotangent.reshape(peer_count, E2_DEV, LATENT)

    def grid_rows_of(slot_ids, device):
        halo = jnp.maximum(slot_ids - G_DEV, 0)
        block = jnp.minimum(halo // HALO_G, 3)
        source = neighbour_device(device, block)
        remote = source * G_DEV + grid_send[source, block, halo % HALO_G]
        return jnp.where(slot_ids < G_DEV, device * G_DEV + slot_ids, remote).astype(jnp.int32)

    def mesh_rows_of(slot_ids, device):
        halo = jnp.maximum(slot_ids - M_DEV, 0)
        block = jnp.minimum(halo // HALO_M, 3)
        source = neighbour_device(device, block)
        near = source * M_DEV + mesh_halo[source, block, halo % HALO_M]
        distant_slot = jnp.maximum(slot_ids - M_DEV - 4 * HALO_M, 0)
        owner = distant_slot // CAP_M
        distant = owner * M_DEV + mesh_send[owner, device, distant_slot % CAP_M]
        return jnp.where(slot_ids < M_DEV, device * M_DEV + slot_ids, jnp.where(slot_ids < M_DEV + 4 * HALO_M, near, distant)).astype(jnp.int32)
    grid_project = product(grid_latent, weights[0]).astype(jnp.bfloat16)
    encode_receive = product(mesh_latent, weights[1]).reshape(peer_count, M_DEV, LATENT)

    def encode_edges(device, slot_ids, targets, receive):
        senders = grid_rows_of(slot_ids, device)
        pre_act = jnp.take(grid_project, senders, axis=0).astype(jnp.float32) + jnp.take(receive, targets, axis=0)
        hidden = jax.nn.silu(pre_act).astype(jnp.bfloat16)
        linear = product(hidden, weights[2])
        return (pre_act, hidden, linear)

    def encode_total(inputs):
        device, slot_ids, targets, receive = inputs
        linear = encode_edges(device, slot_ids, targets, receive)[2]
        message = layer_norm(linear).astype(jnp.bfloat16)
        return jax.ops.segment_sum(message.astype(jnp.float32), targets, num_segments=M_DEV)
    encoder_total = lax.map(encode_total, (device_ids, grid_slots, grid_targets, encode_receive)).reshape(-1, LATENT)
    mesh_middle = (mesh_latent.astype(jnp.float32) + encoder_total).astype(jnp.bfloat16)
    sender_rows = product(mesh_middle, weights[4]).astype(jnp.bfloat16)
    process_receive = product(mesh_middle, weights[5]).reshape(peer_count, M_DEV, LATENT)

    def process_edges(device, slot_ids, targets, receive, edges):
        senders = mesh_rows_of(slot_ids, device)
        pre_act = product(edges, weights[3]) + jnp.take(sender_rows, senders, axis=0).astype(jnp.float32) + jnp.take(receive, targets, axis=0)
        hidden = jax.nn.silu(pre_act).astype(jnp.bfloat16)
        linear = product(hidden, weights[6])
        return (pre_act, hidden, linear)

    def process_total_block(inputs):
        device, slot_ids, targets, receive, edges = inputs
        linear = process_edges(device, slot_ids, targets, receive, edges)[2]
        update = layer_norm(linear).astype(jnp.bfloat16)
        return jax.ops.segment_sum(update.astype(jnp.float32), targets, num_segments=M_DEV)
    process_total = lax.map(process_total_block, (device_ids, mesh_slots, mesh_targets, process_receive, edge_blocks)).reshape(-1, LATENT)
    process_round = process_total.astype(jnp.bfloat16)
    update_pre = product(mesh_middle, weights[7]) + product(process_round, weights[8])
    update_hidden = jax.nn.silu(update_pre).astype(jnp.bfloat16)
    update_linear = product(update_hidden, weights[9])
    mesh_update = (mesh_middle.astype(jnp.float32) + layer_norm(update_linear)).astype(jnp.bfloat16)
    outer_cot = mesh_cotangent.astype(jnp.float32)
    cot_linear = layer_norm_back(update_linear, outer_cot).astype(jnp.bfloat16)
    grad_update_output = outer_sum(update_hidden, cot_linear)
    cot_update = (back_product(cot_linear, weights[9]) * swish_slope(update_pre)).astype(jnp.bfloat16)
    grad_update_self = outer_sum(mesh_middle, cot_update)
    grad_update_message = outer_sum(process_round, cot_update)
    cot_total = back_product(cot_update, weights[8]).reshape(peer_count, M_DEV, LATENT)
    mesh_slot_ids = jnp.arange(mesh_slot_count, dtype=jnp.int32)
    grid_slot_ids = jnp.arange(grid_slot_count, dtype=jnp.int32)

    def process_back(carry, inputs):
        grads_edge, grads_output, sender_acc = carry
        device, slot_ids, targets, receive, edges, edge_cot, total_cot = inputs
        pre_act, hidden, linear = process_edges(device, slot_ids, targets, receive, edges)
        cot_edge = jnp.take(total_cot, targets, axis=0) + edge_cot.astype(jnp.float32)
        cot_plinear = layer_norm_back(linear, cot_edge).astype(jnp.bfloat16)
        grads_output = grads_output + outer_sum(hidden, cot_plinear)
        cot_process = back_product(cot_plinear, weights[6]) * swish_slope(pre_act)
        cot_round = cot_process.astype(jnp.bfloat16)
        grads_edge = grads_edge + outer_sum(edges, cot_round)
        edge_grad_block = (edge_cot.astype(jnp.float32) + back_product(cot_round, weights[3])).astype(jnp.bfloat16)
        cot_receive = jax.ops.segment_sum(cot_process, targets, num_segments=M_DEV).astype(jnp.bfloat16)
        partials = slot_partials(cot_process, slot_ids, mesh_slot_count, M_DEV)
        sender_acc = sender_acc.at[mesh_rows_of(mesh_slot_ids, device)].add(partials)
        return ((grads_edge, grads_output, sender_acc), (edge_grad_block, cot_receive))
    zero_square = jnp.zeros((LATENT, LATENT), jnp.float32)
    start_carry = (zero_square, zero_square, jnp.zeros((M_DEV * peer_count, LATENT), jnp.float32))
    process_carry, process_outs = lax.scan(process_back, start_carry, (device_ids, mesh_slots, mesh_targets, process_receive, edge_blocks, edge_cots, cot_total))
    grad_process_edge, grad_process_output, sender_acc = process_carry
    edge_grad = process_outs[0].reshape(-1, LATENT)
    cot_receive = process_outs[1].reshape(-1, LATENT)
    cot_sender = sender_acc.astype(jnp.bfloat16)
    grad_process_receiver = outer_sum(mesh_middle, cot_receive)
    grad_process_sender = outer_sum(mesh_middle, cot_sender)
    cot_middle = outer_cot + back_product(cot_update, weights[7]) + back_product(cot_receive, weights[5]) + back_product(cot_sender, weights[4])
    cot_blocks = cot_middle.reshape(peer_count, M_DEV, LATENT)

    def encode_back(carry, inputs):
        grads_output, grid_acc = carry
        device, slot_ids, targets, receive, middle_cot = inputs
        pre_act, hidden, linear = encode_edges(device, slot_ids, targets, receive)
        cot_message = jnp.take(middle_cot, targets, axis=0)
        cot_elinear = layer_norm_back(linear, cot_message).astype(jnp.bfloat16)
        grads_output = grads_output + outer_sum(hidden, cot_elinear)
        cot_encoder = back_product(cot_elinear, weights[2]) * swish_slope(pre_act)
        cot_mesh_receive = jax.ops.segment_sum(cot_encoder, targets, num_segments=M_DEV).astype(jnp.bfloat16)
        partials = slot_partials(cot_encoder, slot_ids, grid_slot_count, G_DEV)
        grid_acc = grid_acc.at[grid_rows_of(grid_slot_ids, device)].add(partials)
        return ((grads_output, grid_acc), cot_mesh_receive)
    encode_carry, cot_mesh_receive = lax.scan(encode_back, (zero_square, jnp.zeros((G_DEV * peer_count, LATENT), jnp.float32)), (device_ids, grid_slots, grid_targets, encode_receive, cot_blocks))
    grad_encode_output, grid_acc = encode_carry
    cot_mesh_receive = cot_mesh_receive.reshape(-1, LATENT)
    grad_encode_receiver = outer_sum(mesh_latent, cot_mesh_receive)
    mesh_grad = (cot_middle + back_product(cot_mesh_receive, weights[1])).astype(jnp.bfloat16)
    cot_grid = grid_acc.astype(jnp.bfloat16)
    grad_encode_sender = outer_sum(grid_latent, cot_grid)
    grid_grad = back_product(cot_grid, weights[0]).astype(jnp.bfloat16)
    encode_scale = 1.0 / (E1_DEV * peer_count) ** 0.5
    process_scale = 1.0 / (E2_DEV * peer_count) ** 0.5
    update_scale = 1.0 / (M_DEV * peer_count) ** 0.5
    weight_grads = jnp.stack([grad_encode_sender * encode_scale, grad_encode_receiver * encode_scale, grad_encode_output * encode_scale, grad_process_edge * process_scale, grad_process_sender * process_scale, grad_process_receiver * process_scale, grad_process_output * process_scale, grad_update_self * update_scale, grad_update_message * update_scale, grad_update_output * update_scale]).astype(jnp.bfloat16)
    return (mesh_update, grid_grad, mesh_grad, edge_grad, weight_grads)
```

```python
import jax
import jax.numpy as jnp
from jax import lax
from jax.sharding import PartitionSpec as P

norm_eps = 1e-05


def shifted(value, axis, steps):
    count = lax.axis_size(axis)
    pairs = [(source, (source + steps) % count) for source in range(count)]
    return lax.ppermute(value, axis, pairs)


def layer_norm(values):
    centre = values - jnp.mean(values, axis=-1, keepdims=True)
    spread = jnp.mean(centre * centre, axis=-1, keepdims=True)
    return centre * lax.rsqrt(spread + norm_eps)


def layer_norm_back(values, upstream):
    centre = values - jnp.mean(values, axis=-1, keepdims=True)
    inverse = lax.rsqrt(jnp.mean(centre * centre, axis=-1, keepdims=True) + norm_eps)
    normed = centre * inverse
    return inverse * (
        upstream
        - jnp.mean(upstream, axis=-1, keepdims=True)
        - normed * jnp.mean(upstream * normed, axis=-1, keepdims=True)
    )


def swish_slope(values):
    sigmoid_values = jax.nn.sigmoid(values)
    return sigmoid_values * (1.0 + values * (1.0 - sigmoid_values))


def product(former, latter):
    return jnp.dot(former, latter, preferred_element_type=jnp.float32)


def outer_sum(former, latter):
    return lax.dot_general(
        former, latter, (((0,), (0,)), ((), ())), preferred_element_type=jnp.float32
    )


def back_product(former, latter):
    return lax.dot_general(
        former, latter, (((1,), (1,)), ((), ())), preferred_element_type=jnp.float32
    )


def select_columns(ids, count):
    columns = lax.broadcasted_iota(jnp.int32, (ids.shape[0], count), 1)
    return (ids[:, None] == columns).astype(jnp.bfloat16)


def select_pair(ids, others, count, other_count):
    columns = lax.broadcasted_iota(jnp.int32, (ids.shape[0], count + other_count), 1)
    hit = (ids[:, None] == columns) | ((others + count)[:, None] == columns)
    return hit.astype(jnp.bfloat16)


def stack_grads(terms):
    return jnp.stack([term.astype(jnp.bfloat16) for term in terms])


def grid_neighbours(outgoing):
    from_sub = [shifted(outgoing[block], "sub", offset) for block, offset in ((0, 1), (1, -1))]
    from_face = [shifted(outgoing[block], "face", offset) for block, offset in ((2, 1), (3, -1))]
    return jnp.concatenate(from_sub + from_face, axis=0)


def grid_returns(partials):
    to_sub = [shifted(partials[block], "sub", offset) for block, offset in ((0, -1), (1, 1))]
    to_face = [shifted(partials[block], "face", offset) for block, offset in ((2, -1), (3, 1))]
    return jnp.concatenate(to_sub + to_face, axis=0)


def mesh_neighbours(outgoing):
    from_sub = [shifted(outgoing[block], "sub", offset) for block, offset in ((0, 1), (1, -1))]
    from_face = [shifted(outgoing[block], "face", offset) for block, offset in ((2, 1), (3, -1))]
    return jnp.concatenate(from_sub + from_face, axis=0)


def mesh_returns(partials):
    to_sub = [shifted(partials[block], "sub", offset) for block, offset in ((0, -1), (1, 1))]
    to_face = [shifted(partials[block], "face", offset) for block, offset in ((2, -1), (3, 1))]
    return jnp.concatenate(to_sub + to_face, axis=0)


def move_mesh(outgoing):
    return lax.all_to_all(outgoing, ("face", "sub"), split_axis=0, concat_axis=0, tiled=True)


def return_mesh(outgoing):
    return lax.all_to_all(outgoing, ("face", "sub"), split_axis=0, concat_axis=0, tiled=True)


def on_device(
    grid_latent,
    mesh_latent,
    edge_latent,
    mesh_cotangent,
    edge_cotangent,
    grid_send,
    grid_slot,
    grid_target,
    mesh_halo,
    mesh_send,
    mesh_slot,
    mesh_target,
    weights,
):
    peer_count = lax.axis_size("face") * lax.axis_size("sub")
    latent = weights.shape[1]
    mesh_rows = mesh_latent.shape[0]
    grid_rows = grid_latent.shape[0]
    grid_table = grid_send[0].reshape(-1)
    halo_table = mesh_halo[0].reshape(-1)
    far_table = mesh_send[0].reshape(-1)
    halo_count = halo_table.shape[0]
    slot_count = mesh_rows + halo_count + far_table.shape[0]
    grid_slot_count = grid_rows + grid_table.shape[0]
    pick_grid = select_columns(grid_table, grid_rows)
    pick_halo_far = select_columns(jnp.concatenate([halo_table, far_table]), mesh_rows)
    grid_pair = select_pair(grid_slot, grid_target, grid_slot_count, mesh_rows)
    mesh_pair = select_pair(mesh_slot, mesh_target, slot_count, mesh_rows)
    grid_onehot = select_columns(grid_target, mesh_rows)
    mesh_onehot = select_columns(mesh_target, mesh_rows)
    encode_scale = 1.0 / (grid_slot.shape[0] * peer_count) ** 0.5
    process_scale = 1.0 / (mesh_slot.shape[0] * peer_count) ** 0.5
    update_scale = 1.0 / (mesh_rows * peer_count) ** 0.5
    grid_project = product(grid_latent, weights[0]).astype(jnp.bfloat16)
    grid_outgoing = (
        product(pick_grid, grid_project).astype(jnp.bfloat16).reshape(4, -1, latent)
    )
    encode_receive = product(mesh_latent, weights[1]).astype(jnp.bfloat16)
    grid_source = jnp.concatenate(
        [grid_project, grid_neighbours(grid_outgoing), encode_receive], axis=0
    )
    encoder_pre = product(grid_pair, grid_source)
    encoder_hidden = jax.nn.silu(encoder_pre).astype(jnp.bfloat16)
    encoder_linear = product(encoder_hidden, weights[2])
    encoder_message = layer_norm(encoder_linear).astype(jnp.bfloat16)
    encoder_total = outer_sum(grid_onehot, encoder_message)
    mesh_middle = (mesh_latent.astype(jnp.float32) + encoder_total).astype(jnp.bfloat16)
    sender_rows = product(mesh_middle, weights[4]).astype(jnp.bfloat16)
    outgoing = product(pick_halo_far, sender_rows).astype(jnp.bfloat16)
    halo_outgoing = outgoing[:halo_count].reshape(4, -1, latent)
    far_outgoing = outgoing[halo_count:].reshape(peer_count, -1, latent)
    far_incoming = move_mesh(far_outgoing).reshape(-1, latent)
    process_receive = product(mesh_middle, weights[5]).astype(jnp.bfloat16)
    mesh_source = jnp.concatenate(
        [sender_rows, mesh_neighbours(halo_outgoing), far_incoming, process_receive], axis=0
    )
    process_pre = product(edge_latent, weights[3]) + product(mesh_pair, mesh_source)
    process_hidden = jax.nn.silu(process_pre).astype(jnp.bfloat16)
    process_linear = product(process_hidden, weights[6])
    edge_update = layer_norm(process_linear).astype(jnp.bfloat16)
    process_round = outer_sum(mesh_onehot, edge_update).astype(jnp.bfloat16)
    update_pre = product(mesh_middle, weights[7]) + product(process_round, weights[8])
    update_hidden = jax.nn.silu(update_pre).astype(jnp.bfloat16)
    update_linear = product(update_hidden, weights[9])
    mesh_update = (mesh_middle.astype(jnp.float32) + layer_norm(update_linear)).astype(jnp.bfloat16)
    outer_cot = mesh_cotangent.astype(jnp.float32)
    cot_linear = layer_norm_back(update_linear, outer_cot).astype(jnp.bfloat16)
    grad_update_output = outer_sum(update_hidden, cot_linear)
    cot_update = (back_product(cot_linear, weights[9]) * swish_slope(update_pre)).astype(
        jnp.bfloat16
    )
    grad_update_self = outer_sum(mesh_middle, cot_update)
    grad_update_message = outer_sum(process_round, cot_update)
    cot_total = back_product(cot_update, weights[8]).astype(jnp.bfloat16)
    edge_cot = edge_cotangent.astype(jnp.float32)
    cot_edge = product(mesh_onehot, cot_total) + edge_cot
    cot_plinear = layer_norm_back(process_linear, cot_edge).astype(jnp.bfloat16)
    grad_process_output = outer_sum(process_hidden, cot_plinear)
    cot_process = back_product(cot_plinear, weights[6]) * swish_slope(process_pre)
    cot_round = cot_process.astype(jnp.bfloat16)
    grad_process_edge = outer_sum(edge_latent, cot_round)
    edge_grad = (edge_cot + back_product(cot_round, weights[3])).astype(jnp.bfloat16)
    cot_slot = outer_sum(mesh_pair, cot_round)
    cot_receive = cot_slot[slot_count:].astype(jnp.bfloat16)
    grad_process_receiver = outer_sum(mesh_middle, cot_receive)
    halo_partials = (
        cot_slot[mesh_rows : mesh_rows + halo_count].astype(jnp.bfloat16).reshape(4, -1, latent)
    )
    far_partials = (
        cot_slot[mesh_rows + halo_count : slot_count].astype(jnp.bfloat16).reshape(peer_count, -1, latent)
    )
    far_returned = return_mesh(far_partials).reshape(-1, latent)
    returned = jnp.concatenate([mesh_returns(halo_partials), far_returned], axis=0)
    sender_total = cot_slot[:mesh_rows] + outer_sum(pick_halo_far, returned)
    cot_sender = sender_total.astype(jnp.bfloat16)
    grad_process_sender = outer_sum(mesh_middle, cot_sender)
    cot_middle = (
        outer_cot
        + back_product(cot_update, weights[7])
        + back_product(cot_receive, weights[5])
        + back_product(cot_sender, weights[4])
    )
    process_grads = stack_grads(
        [
            grad_process_edge,
            grad_process_sender,
            grad_process_receiver,
            grad_process_output,
            grad_update_self,
            grad_update_message,
            grad_update_output,
        ]
    )
    process_grads = lax.psum(process_grads, ("face", "sub"))
    cot_message = product(grid_onehot, cot_middle.astype(jnp.bfloat16))
    cot_elinear = layer_norm_back(encoder_linear, cot_message).astype(jnp.bfloat16)
    grad_encode_output = outer_sum(encoder_hidden, cot_elinear)
    cot_encoder = back_product(cot_elinear, weights[2]) * swish_slope(encoder_pre)
    cot_gslot = outer_sum(grid_pair, cot_encoder.astype(jnp.bfloat16))
    cot_mesh_receive = cot_gslot[grid_slot_count:].astype(jnp.bfloat16)
    grad_encode_receiver = outer_sum(mesh_latent, cot_mesh_receive)
    mesh_grad = (cot_middle + back_product(cot_mesh_receive, weights[1])).astype(jnp.bfloat16)
    grid_partials = cot_gslot[grid_rows:grid_slot_count].astype(jnp.bfloat16).reshape(4, -1, latent)
    grid_returned = grid_returns(grid_partials)
    cot_grid = (cot_gslot[:grid_rows] + outer_sum(pick_grid, grid_returned)).astype(jnp.bfloat16)
    grad_encode_sender = outer_sum(grid_latent, cot_grid)
    grid_grad = back_product(cot_grid, weights[0]).astype(jnp.bfloat16)
    encode_grads = stack_grads([grad_encode_sender, grad_encode_receiver, grad_encode_output])
    encode_grads, process_grads = lax.optimization_barrier((encode_grads, process_grads))
    encode_grads = lax.psum(encode_grads, ("face", "sub"))
    summed = jnp.concatenate([encode_grads, process_grads], axis=0).astype(jnp.float32)
    scale_column = jnp.array(
        [encode_scale] * 3 + [process_scale] * 4 + [update_scale] * 3, jnp.float32
    )
    weight_grads = (summed * scale_column[:, None, None]).astype(jnp.bfloat16)
    return (mesh_update, grid_grad, mesh_grad, edge_grad, weight_grads)


def solution(mesh):
    return jax.shard_map(
        on_device,
        mesh=mesh,
        in_specs=(
            P(("face", "sub"), None),
            P(("face", "sub"), None),
            P(("face", "sub"), None),
            P(("face", "sub"), None),
            P(("face", "sub"), None),
            P(("face", "sub"), None, None),
            P(("face", "sub")),
            P(("face", "sub")),
            P(("face", "sub"), None, None),
            P(("face", "sub"), None, None),
            P(("face", "sub")),
            P(("face", "sub")),
            P(),
        ),
        out_specs=(
            P(("face", "sub"), None),
            P(("face", "sub"), None),
            P(("face", "sub"), None),
            P(("face", "sub"), None),
            P(),
        ),
        check_vma=False,
    )
```
